32 devices in a mesh: dp: 16 (over z, x, core), mp: 2 (over y).
Axes of the slice: x: 2, y: 2, z: 4, core: 2. Of those that a mesh axis runs over, the one named last changes fastest.
Arguments:
- queries: bfloat16 [12288, 1024], P('dp', 'mp'), may hold values from -3 to 3
- passages: bfloat16 [12288, 1024], P('dp', 'mp'), may hold values from -3 to 3
- positive: int32 [12288], P('dp'), may hold values from 0 to 12287
Outputs:
- grad_queries: bfloat16 [12288, 1024], P('dp', 'mp')
- grad_passages: bfloat16 [12288, 1024], P('dp', 'mp')
The draws below stay inside these ranges and needn't reach their ends.
All inputs are finite; a program needn't handle non-finite values.
Results may differ from the reference program's by a relative error of at most 0.0034.
Values may be sent and summed in bfloat16 or wider, within the bound.
A program may use at most 128 MiB of HBM per device.

```python
import math
import jax
import jax.numpy as jnp
from jax import lax

D = 1024
PAIRS = 12288


def paired_draw(key):
    inner = jax.random.fold_in(key, 11)
    first_key, second_key, third_key = jax.random.split(inner, 3)
    query_vals = jnp.clip(jax.random.normal(first_key, (PAIRS, D), jnp.float32), -3.0, 3.0)
    passage_vals = jnp.clip(jax.random.normal(second_key, (PAIRS, D), jnp.float32), -3.0, 3.0)
    return (query_vals.astype(jnp.bfloat16), passage_vals.astype(jnp.bfloat16))


def draw_queries(key, part):
    return paired_draw(key)[0]


def draw_passages(key, part):
    return paired_draw(key)[1]


def place_ends(drawn, key, least, high):
    shape = drawn.shape
    place = [jax.random.randint(jax.random.fold_in(key, axis), (), 0, shape[axis]) for axis in range(len(shape))]
    drawn = drawn.at[tuple(place)].set(least)
    longest = shape.index(max(shape))
    place[longest] = (place[longest] + 1) % shape[longest]
    return drawn.at[tuple(place)].set(high)


def setup_inputs(seed: int = 0) -> dict:
    key_of = jax.random.split(jax.random.key(seed), 4)
    return {
        "queries": draw_queries(jax.random.fold_in(key_of[3], 71), 0),
        "passages": draw_passages(jax.random.fold_in(key_of[3], 71), 0),
        "positive": place_ends(jax.random.randint(key_of[2], (PAIRS,), 0, PAIRS), jax.random.fold_in(key_of[2], 1), 0, PAIRS - 1).astype(jnp.int32),
    }


def reference(queries, passages, positive):
    logit_scale = 3.0 / math.sqrt(D)
    block_rows = math.gcd(PAIRS, 512)
    block_count = PAIRS // block_rows
    query_blocks = queries.reshape(block_count, block_rows, D)
    target_blocks = positive.reshape(block_count, block_rows)
    column_ids = jnp.arange(PAIRS, dtype=jnp.int32)

    def one_block(carried, inputs):
        query_rows, targets = inputs
        scores = jnp.dot(query_rows, passages.T, preferred_element_type=jnp.float32) * logit_scale
        highest = lax.optimization_barrier(jnp.max(scores, axis=1))
        log_total = highest + jnp.log(lax.optimization_barrier(jnp.sum(jnp.exp(scores - highest[:, None]), axis=1)))
        onehot = (column_ids[None, :] == targets[:, None]).astype(jnp.float32)
        softmax_grad = (jnp.exp(scores - log_total[:, None]) - onehot).astype(jnp.bfloat16)
        query_grad = jnp.dot(softmax_grad, passages, preferred_element_type=jnp.float32).astype(jnp.bfloat16)
        carried = carried + jnp.dot(softmax_grad.T, query_rows, preferred_element_type=jnp.float32)
        return (carried, query_grad)
    start_grad = jnp.zeros((PAIRS, D), jnp.float32)
    passage_total, query_grads = lax.scan(one_block, start_grad, (query_blocks, target_blocks))
    return (query_grads.reshape(PAIRS, D), passage_total.astype(jnp.bfloat16))
```

```python
import math

import jax
import jax.numpy as jnp
from jax import lax
from jax.sharding import PartitionSpec as P


def reduce_width(terms):
    count = lax.axis_size("mp")
    index = lax.axis_index("mp")
    width = terms.shape[1] // count
    total = lax.dynamic_slice_in_dim(terms, index * width, width, 1)
    for hop in range(1, count):
        sent = lax.dynamic_slice_in_dim(terms, (index + hop) % count * width, width, 1)
        ring = [(d, (d + hop) % count) for d in range(count)]
        total += lax.ppermute(sent.astype(jnp.bfloat16), "mp", ring).astype(jnp.float32)
    return total.astype(jnp.bfloat16)


def local(queries, passages, positive):
    group_rows, slice_width = queries.shape
    group_count = lax.axis_size("dp")
    model_index = lax.axis_index("mp")
    relaid = lax.all_to_all(passages, "mp", split_axis=0, concat_axis=1, tiled=True)
    short_rows = relaid.shape[0]
    wide_queries = lax.all_gather(queries, "mp", axis=1, tiled=True)
    passage_block = lax.all_gather(relaid, "dp", axis=0, tiled=True)
    full_width = wide_queries.shape[1]
    logit_scale = 3.0 / math.sqrt(full_width)
    scores = (
        lax.dot_general(
            wide_queries,
            passage_block,
            (((1,), (1,)), ((), ())),
            preferred_element_type=jnp.float32,
        )
        * logit_scale
    )
    local_max = jnp.max(scores, axis=1)
    highest = lax.pmax(local_max, "mp")
    row_total = lax.psum(jnp.sum(jnp.exp(scores - highest[:, None]), axis=1), "mp")
    log_total = highest + jnp.log(row_total)
    column_pos = jnp.arange(group_count * short_rows, dtype=jnp.int32)
    column_ids = (
        column_pos // short_rows * group_rows + model_index * short_rows + column_pos % short_rows
    )
    onehot = (column_ids[None, :] == positive[:, None]).astype(jnp.float32)
    softmax_grad = (jnp.exp(scores - log_total[:, None]) - onehot).astype(jnp.bfloat16)
    query_terms = jnp.dot(softmax_grad, passage_block, preferred_element_type=jnp.float32)
    grad_queries = reduce_width(query_terms)
    group_index = lax.axis_index("dp")
    own_passages = lax.all_gather(passages, "mp", axis=1, tiled=True)
    query_relaid = lax.all_to_all(queries, "mp", split_axis=0, concat_axis=1, tiled=True)
    all_queries = lax.all_gather(query_relaid, "dp", axis=0, tiled=True)
    own_log = lax.dynamic_slice_in_dim(log_total, model_index * short_rows, short_rows)
    own_targets = lax.dynamic_slice_in_dim(positive, model_index * short_rows, short_rows).astype(
        jnp.float32
    )
    all_log, all_targets = (
        lax.all_gather(own_log, "dp", axis=0, tiled=True),
        lax.all_gather(own_targets, "dp", axis=0, tiled=True),
    )
    own_scores = (
        lax.dot_general(
            all_queries, own_passages, (((1,), (1,)), ((), ())), preferred_element_type=jnp.float32
        )
        * logit_scale
    )
    own_ids = (group_index * group_rows + jnp.arange(group_rows, dtype=jnp.int32)).astype(
        jnp.float32
    )
    own_hits = (own_ids[None, :] == all_targets[:, None]).astype(jnp.float32)
    own_grad = (jnp.exp(own_scores - all_log[:, None]) - own_hits).astype(jnp.bfloat16)
    own_terms = lax.dot_general(
        own_grad, all_queries, (((0,), (0,)), ((), ())), preferred_element_type=jnp.float32
    )
    grad_passages = reduce_width(own_terms)
    return (grad_queries, grad_passages)


def solution(mesh):
    return jax.shard_map(
        local,
        mesh=mesh,
        in_specs=(P("dp", "mp"), P("dp", "mp"), P("dp")),
        out_specs=(P("dp", "mp"), P("dp", "mp")),
        check_vma=False,
    )
```
